16 devices in a mesh: rep: 1, dp: 16 (over x, y, z, core).
Axes of the slice: x: 2, y: 2, z: 2, core: 2. Of those that a mesh axis runs over, the one named last changes fastest.
Arguments:
- x: bfloat16 [16, 2048, 1024], P(('rep', 'dp'))
- dy: bfloat16 [16, 2048, 1024], P(('rep', 'dp'))
- w_gate: bfloat16 [2, 1024, 3200], P(None, 'dp')
- w_up: bfloat16 [2, 1024, 3200], P(None, 'dp')
- w_down: bfloat16 [2, 3200, 1024], P(None, 'dp')
- m_w_gate: float32 [2, 1024, 3200], P(None, 'dp')
- m_w_up: float32 [2, 1024, 3200], P(None, 'dp')
- m_w_down: float32 [2, 3200, 1024], P(None, 'dp')
- v_w_gate: float32 [2, 1024, 3200], P(None, 'dp')
- v_w_up: float32 [2, 1024, 3200], P(None, 'dp')
- v_w_down: float32 [2, 3200, 1024], P(None, 'dp')
Outputs:
- output 1: bfloat16 [2, 1024, 3200], P('rep', 'dp')
- output 2: bfloat16 [2, 1024, 3200], P('rep', 'dp')
- output 3: bfloat16 [2, 3200, 1024], P('rep', 'dp')
- output 4: float32 [2, 1024, 3200], P('rep', 'dp')
- output 5: float32 [2, 1024, 3200], P('rep', 'dp')
- output 6: float32 [2, 3200, 1024], P('rep', 'dp')
- output 7: float32 [2, 1024, 3200], P('rep', 'dp')
- output 8: float32 [2, 1024, 3200], P('rep', 'dp')
- output 9: float32 [2, 3200, 1024], P('rep', 'dp')
All inputs are finite; a program needn't handle non-finite values.
Results may differ from the reference program's by a relative error of at most 0.0223.
Values are sent between devices in bfloat16 or wider.
A program may use at most 2 GiB of HBM per device.

```python
import jax
import jax.numpy as jnp
from jax import lax

SEQUENCES = 16
TOKENS = 2048
D = 1024
FF = 3200
LAYERS = 2
NAMES = ("w_gate", "w_up", "w_down")
SHAPES = {"w_gate": (LAYERS, D, FF), "w_up": (LAYERS, D, FF), "w_down": (LAYERS, FF, D)}


def bump(key, n, height):
    away = (jnp.arange(n, dtype=jnp.int32) - jax.random.randint(key, (), 0, n, jnp.int32)) % n
    return jnp.where(away < n // 8, height, 1.0)


def together(key, own, strength):
    shared = jax.random.normal(key, own.shape[1:], jnp.float32)
    return (own + strength * shared) * lax.rsqrt(1 + strength * strength)


def setup_inputs(seed: int = 0, part: int = 0) -> dict:
    kx, kdy, ka, kb, kz, kf, kh, kl, *keys = jax.random.split(jax.random.key(seed), 8 + 3 * len(NAMES))
    kx, kdy, ka, kb = (jax.random.fold_in(k, part) for k in (kx, kdy, ka, kb))
    kw, km, kv = (keys[i::3] for i in range(3))
    shape = (SEQUENCES, TOKENS, D)
    much_x, much_dy = jax.random.uniform(kz, (2,), jnp.float32, 0.0, 1.0)
    loud = 2.0 ** jax.random.uniform(jax.random.fold_in(kz, 1), (), jnp.float32, -1.0, 2.0)
    layers = 2.0 ** jax.random.uniform(kl, (LAYERS, 1, 1), jnp.float32, -1.0, 1.0)
    x = together(ka, jax.random.normal(kx, shape, jnp.float32), much_x) * bump(kf, D, 4.0)
    dy = together(kb, jax.random.normal(kdy, shape, jnp.float32), much_dy)
    drawn = {"x": x.astype(jnp.bfloat16), "dy": (loud * dy * (SEQUENCES * TOKENS) ** -0.5).astype(jnp.bfloat16)}
    for key, name in zip(kw, NAMES, strict=True):
        w = jax.random.normal(key, SHAPES[name], jnp.float32) * SHAPES[name][1] ** -0.5
        drawn[name] = (w * {"w_gate": 1.0, "w_up": bump(kh, FF, 4.0), "w_down": layers}[name]).astype(jnp.bfloat16)
    for key, name in zip(km, NAMES, strict=True):
        drawn[f"m_{name}"] = 0.1 * jax.random.normal(key, SHAPES[name], jnp.float32)
    for key, name in zip(kv, NAMES, strict=True):
        drawn[f"v_{name}"] = jax.random.uniform(key, SHAPES[name], jnp.float32, 0.005, 0.015)
    return drawn


def matmul(a, w):
    return jnp.dot(a, w, preferred_element_type=jnp.float32).astype(jnp.bfloat16)


def normed(h):
    wide = h.astype(jnp.float32)
    scale = lax.rsqrt(jnp.mean(wide**2, -1, keepdims=True) + 1e-6)
    return (wide * scale).astype(jnp.bfloat16)


def layer(h, w):
    a = normed(h)
    gate = jnp.dot(a, w["w_gate"], preferred_element_type=jnp.float32)
    up = jnp.dot(a, w["w_up"], preferred_element_type=jnp.float32)
    return h + matmul((jax.nn.silu(gate) * up).astype(jnp.bfloat16), w["w_down"])


def adamw(w, m, v, g):
    m = 0.9 * m + 0.1 * g
    v = 0.95 * v + 0.05 * g * g
    step = m * lax.rsqrt(v + 1e-8) + 0.1 * w
    return (w - 0.02 * step).astype(jnp.bfloat16), m, v


def clipped(gradients, sum_of_squares, count):
    factor = jnp.minimum(1.0, 0.5 * lax.rsqrt(sum_of_squares / count + 1e-30))
    return [g * factor for g in gradients]


def stack(weights, h):
    return lax.scan(lambda h, w: (layer(h, w), None), h, weights)[0]


def reference(x, dy, w_gate, w_up, w_down, m_w_gate, m_w_up, m_w_down, v_w_gate, v_w_up, v_w_down):
    weights = dict(zip(NAMES, (w_gate, w_up, w_down), strict=True))

    def take(so_far, sequence):
        h, by_y = sequence
        _, back = jax.vjp(lambda w: stack(w, h), weights)
        return jax.tree.map(lambda total, term: total + term.astype(jnp.float32), so_far, back(by_y)[0]), None

    none_yet = {name: jnp.zeros(w.shape, jnp.float32) for name, w in weights.items()}
    by_weights, _ = lax.scan(take, none_yet, (x, dy))
    gradients = [by_weights[name].astype(jnp.bfloat16).astype(jnp.float32) for name in NAMES]
    gradients = clipped(gradients, sum(jnp.sum(g * g) for g in gradients), sum(g.size for g in gradients))
    new = [
        adamw(w.astype(jnp.float32), m, v, g)
        for w, m, v, g in zip((w_gate, w_up, w_down), (m_w_gate, m_w_up, m_w_down), (v_w_gate, v_w_up, v_w_down), gradients, strict=True)
    ]
    return tuple(one[which] for which in range(3) for one in new)
```

```python
import functools

import jax
import jax.numpy as jnp
from jax import lax
from jax.experimental import pallas as pl
from jax.experimental.pallas import tpu as pltpu
from jax.sharding import PartitionSpec as P

BF, F32 = jnp.bfloat16, jnp.float32
ALL = pl.BlockSpec(memory_space=pl.ANY)
DMA = pltpu.SemaphoreType.DMA


def position():
    me = lax.axis_index("dp")
    return [(me // w) % 2 for w in (8, 4, 2, 1)], me


def across(bits, me, axis):
    w = (8, 4, 2, 1)[axis]
    return {"dp": me + w - 2 * w * bits[axis]}


def greet(bits, me):
    barrier = pltpu.get_barrier_semaphore()
    for axis in range(4):
        pl.semaphore_signal(barrier, inc=1, device_id=across(bits, me, axis), device_id_type=pl.DeviceIdType.MESH)
    pl.semaphore_wait(barrier, 4)


def parts_of(columns, pieces):
    lanes, n = columns // 128, 3 * pieces
    cuts = [128 * (lanes * i // n) for i in range(n + 1)]
    return [[(cuts[3 * j + p], cuts[3 * j + p + 1] - cuts[3 * j + p], ((0, 1, 2), (1, 2, 0), (2, 0, 1))[p]) for p in range(3)] for j in range(pieces)]


class Gather:
    def __init__(self, source, layer):
        self.source, self.layer = source, layer
        self.rows, self.columns = source.shape[1:]
        self.parts = parts_of(self.columns, 1)[0]
        self.inputs = [source]
        self.outputs = [jax.ShapeDtypeStruct((2, 2, 2, 2, self.rows, self.columns), BF)]
        self.out_specs = [ALL]
        self.scratch = [pltpu.VMEM((self.rows, self.columns), BF), DMA((2,)), DMA((3, 3)), DMA((3, 3)), DMA((10,)), DMA((10,))]

    def phases(self, inputs, outputs, scratch):
        (source,), (out,), (own, local, send, recv, csend, crecv) = inputs, outputs, scratch
        bits, me = position()

        def region(flipped, both):
            return tuple(slice(None) if a in both else (1 - bits[a] if a in flipped else bits[a]) for a in range(4))

        def hop(stage, p):
            c0, n, order = self.parts[p]
            where = region((), order[:stage]) + (slice(None), pl.ds(c0, n))
            src = own.at[:, pl.ds(c0, n)] if stage == 0 else out.at[where]
            return pltpu.make_async_remote_copy(src, out.at[where], send.at[stage, p], recv.at[stage, p], device_id=across(bits, me, order[stage]), device_id_type=pl.DeviceIdType.MESH)

        def pass_on(stage, p):
            if stage < 0:
                where, src, slot = region((), ()), own, 9
            else:
                c0, n, order = self.parts[p]
                where = region((order[stage],), order[:stage]) + (slice(None), pl.ds(c0, n))
                src, slot = out.at[where], 3 * stage + p
            return pltpu.make_async_remote_copy(src, out.at[where], csend.at[slot], crecv.at[slot], device_id=across(bits, me, 3), device_id_type=pl.DeviceIdType.MESH)

        load = pltpu.make_async_copy(source.at[self.layer], own, local.at[0])
        store = pltpu.make_async_copy(own, out.at[tuple(bits)], local.at[1])

        def first():
            load.start()
            greet(bits, me)
            load.wait()
            for p in range(3):
                hop(0, p).start()
            store.start()
            pass_on(-1, 0).start()

        def middle(stage):
            if stage == 1:
                store.wait()
            for p in range(3):
                hop(stage - 1, p).wait_recv()
                if stage < 3:
                    hop(stage, p).start()
                pass_on(stage - 1, p).start()

        def last():
            for stage in range(3):
                for p in range(3):
                    hop(stage, p).wait_send()
                    pass_on(stage, p).wait()
            pass_on(-1, 0).wait()

        return [first] + [functools.partial(middle, s) for s in (1, 2, 3)] + [last]


class Scatter:
    def __init__(self, g, pieces=2):
        self.rows, self.columns = g.shape[4:]
        self.pieces = parts_of(self.columns, pieces)
        self.inputs = [g]
        r, c, n = self.rows, self.columns, pieces
        self.outputs = [jax.ShapeDtypeStruct((r, c), BF)]
        self.out_specs = [pl.BlockSpec((r, c), lambda *_: (0, 0))]
        buffers = [(2, 2, 2, r, c), (2, 2, 2, r, c), (2, 2, r, c), (2, r, c), (r, c), (2, 2, r, c), (2, r, c), (r, c)]
        self.scratch = [pltpu.VMEM(b, BF) for b in buffers] + [DMA((n,)), DMA((n, 2)), DMA((n, 3, 3)), DMA((n, 3, 3))]

    def phases(self, inputs, outputs, scratch):
        (g,), (out,) = inputs, outputs
        keep, far, in1, in2, in3, out1, out2, out3, local, core, send, recv = scratch
        ins, outs = (in1, in2, in3), (out1, out2, out3)
        bits, me = position()

        def columns_of(j):
            parts = self.pieces[j]
            return pl.ds(parts[0][0], sum(n for _, n, _ in parts))

        def load(j):
            at = columns_of(j)
            return pltpu.make_async_copy(g.at[:, :, :, bits[3], :, at], keep.at[:, :, :, :, at], local.at[j])

        def swap(j):
            at = columns_of(j)
            return pltpu.make_async_remote_copy(g.at[:, :, :, 1 - bits[3], :, at], far.at[:, :, :, :, at], core.at[j, 0], core.at[j, 1], device_id=across(bits, me, 3), device_id_type=pl.DeviceIdType.MESH)

        def hop(j, p, stage):
            c0, n, order = self.pieces[j][p]
            at = (slice(None),) * (2 - stage) + (slice(None), pl.ds(c0, n))
            return pltpu.make_async_remote_copy(outs[stage].at[at], ins[stage].at[at], send.at[j, p, stage], recv.at[j, p, stage], device_id=across(bits, me, order[stage]), device_id_type=pl.DeviceIdType.MESH)

        def total(part, stage, block):
            c0, n, order = part
            at = pl.ds(c0, n)
            xyz = [None] * 3
            for a, b in zip(order, block):
                xyz[a] = b
            where = tuple(xyz) + (slice(None), at)
            t = keep[where].astype(F32) + far[where].astype(F32)
            for s in range(stage):
                t = t + ins[s][tuple(block[s + 1 :]) + (slice(None), at)].astype(F32)
            return t

        def first():
            greet(bits, me)
            for j in range(len(self.pieces)):
                swap(j).start()
                load(j).start()

        def stage_of(j, stage):
            if stage == 0:
                load(j).wait()
                swap(j).wait_recv()
            for p, part in enumerate(self.pieces[j]):
                c0, n, order = part
                b = [bits[a] for a in order]
                if stage:
                    hop(j, p, stage - 1).wait_recv()
                if stage == 3:
                    out[:, pl.ds(c0, n)] = total(part, 3, b).astype(BF)
                    continue
                if stage == 2:
                    out3[:, pl.ds(c0, n)] = total(part, 2, b[:2] + [1 - b[2]]).astype(BF)
                else:
                    @pl.loop(0, 4 if stage == 0 else 2)
                    def _(i):
                        rest = [i // 2, i % 2] if stage == 0 else [i]
                        block = b[:stage] + [1 - b[stage]] + rest
                        outs[stage][tuple(rest) + (slice(None), pl.ds(c0, n))] = total(part, stage, block).astype(BF)
                hop(j, p, stage).start()

        def last():
            for j in range(len(self.pieces)):
                swap(j).wait_send()
                for p in range(3):
                    for stage in range(3):
                        hop(j, p, stage).wait_send()

        middle = [functools.partial(stage_of, j, s) for s in range(4) for j in range(len(self.pieces))]
        return [first] + middle + [last]


def kernel(name, number, grid, compute, inputs, in_specs, outputs, out_specs, scratch=(), comm=None, schedule=(), flops=0, bytes_accessed=0):
    n_in, n_out = len(inputs), len(outputs)
    c_in, c_out, c_scratch = (comm.inputs, comm.outputs, comm.scratch) if comm else ([], [], [])

    def body(*refs):
        step = pl.program_id(0)
        i, o = refs[:n_in], refs[n_in + len(c_in) : n_in + len(c_in) + n_out]
        rest = refs[n_in + len(c_in) + n_out + len(c_out) :]
        phases = []
        if comm:
            phases = comm.phases(refs[n_in : n_in + len(c_in)], refs[n_in + len(c_in) + n_out :][: len(c_out)], rest[len(scratch) :])
        for k, phase in enumerate(phases):
            if k < len(schedule):
                pl.when(step == schedule[k])(phase)
        if compute:
            compute(step, i, o, rest[: len(scratch)])
        if len(phases) > len(schedule):
            @pl.when(step == grid - 1)
            def _():
                for phase in phases[len(schedule) :]:
                    phase()

    return pl.pallas_call(
        body,
        grid=(grid,),
        out_shape=list(outputs) + c_out,
        in_specs=list(in_specs) + [ALL] * len(c_in),
        out_specs=list(out_specs) + (comm.out_specs if comm else []),
        scratch_shapes=list(scratch) + c_scratch,
        compiler_params=pltpu.CompilerParams(
            dimension_semantics=("arbitrary",),
            collective_id=number if comm else None,
            has_side_effects=bool(comm),
            vmem_limit_bytes=60 << 20,
        ),
        cost_estimate=pl.CostEstimate(flops=flops, bytes_accessed=bytes_accessed, transcendentals=0),
        name=name,
    )(*inputs, *c_in)
NAMES = ("w_gate", "w_up", "w_down")
TILE = 256
TURNED = (((1,), (1,)), ((), ()))
SUMMED = (((0,), (0,)), ((), ()))


def chunks(n, size=768):
    starts = list(range(0, n - size + 1, size))
    return [(s, (n if s == starts[-1] else s + size) - s) for s in starts]


def dot(a, b):
    return jnp.dot(a, b, preferred_element_type=F32)


def dot_turned(a, b):
    return lax.dot_general(a, b, TURNED, preferred_element_type=F32)


def rows(columns):
    return pl.BlockSpec((TILE, columns), lambda s: (s, 0))


def whole(shape):
    return pl.BlockSpec(shape, lambda s: (0, 0), pipeline_mode=pl.Buffered(1))


def gate_kernel(number, h, w, comm=None, schedule=()):
    (tokens, d), f = h.shape, w.shape[1]

    def compute(step, i, o, _):
        h_ref, w_ref = i
        a_ref, gate_ref = o
        wide = h_ref[...].astype(F32)
        a = (wide * lax.rsqrt(jnp.mean(wide**2, -1, keepdims=True) + 1e-6)).astype(BF)
        a_ref[...] = a
        for c, n in chunks(f):
            gate_ref[:, c : c + n] = dot(a, w_ref[:, c : c + n])

    outs = [jax.ShapeDtypeStruct((tokens, d), BF), jax.ShapeDtypeStruct((tokens, f), F32)]
    return kernel(f"gate{number}", number, tokens // TILE, compute, [h, w], [rows(d), whole(w.shape)], outs, [rows(d), rows(f)], (), comm, schedule, 2 * tokens * d * f)


def up_kernel(number, a, w, gate, comm=None, schedule=()):
    (tokens, d), f = a.shape, w.shape[1]

    def compute(step, i, o, _):
        a_ref, w_ref, gate_ref = i
        up_ref, act_ref = o
        for c, n in chunks(f):
            at = slice(c, c + n)
            up = dot(a_ref[...], w_ref[:, at])
            up_ref[:, at] = up
            gate = gate_ref[:, at]
            act_ref[:, at] = (gate * jax.nn.sigmoid(gate) * up).astype(BF)

    outs = [jax.ShapeDtypeStruct((tokens, f), F32), jax.ShapeDtypeStruct((tokens, f), BF)]
    return kernel(f"up{number}", number, tokens // TILE, compute, [a, w, gate], [rows(d), whole(w.shape), rows(f)], outs, [rows(f), rows(f)], (), comm, schedule, 2 * tokens * d * f)


def down_kernel(number, act, w, h, comm=None, schedule=()):
    (tokens, f), d = act.shape, w.shape[1]

    def compute(step, i, o, _):
        act_ref, w_ref, h_ref = i
        product = dot(act_ref[...], w_ref[...]).astype(BF)
        o[0][...] = (h_ref[...].astype(F32) + product.astype(F32)).astype(BF)

    outs = [jax.ShapeDtypeStruct((tokens, d), BF)]
    return kernel(f"down{number}", number, tokens // TILE, compute, [act, w, h], [rows(f), whole(w.shape), rows(d)], outs, [rows(d)], (), comm, schedule, 2 * tokens * d * f)


def gated_back(by_act, gate, up):
    s = jax.nn.sigmoid(gate)
    silu = gate * s
    return (by_act * up * (s + silu * (1.0 - s))).astype(BF), (by_act * silu).astype(BF), silu


def hidden_back_kernel(number, by_y, w, comm=None, schedule=()):
    (tokens, d), f = by_y.shape, w.shape[0]

    def compute(step, i, o, _):
        for c, n in chunks(f):
            o[0][:, c : c + n] = dot_turned(i[0][...], i[1][c : c + n, :]).astype(BF)

    outs = [jax.ShapeDtypeStruct((tokens, f), BF)]
    return kernel(f"hidden_back{number}", number, tokens // TILE, compute, [by_y, w], [rows(d), whole(w.shape)], outs, [rows(f)], (), comm, schedule, 2 * tokens * d * f)


def up_back_kernel(number, a, w, gate, by_act, comm=None, schedule=()):
    (tokens, d), f = a.shape, w.shape[1]

    def compute(step, i, o, _):
        a_ref, w_ref, gate_ref, by_ref = i
        act_ref, by_gate_ref, by_up_ref = o
        for c, n in chunks(f):
            at = slice(c, c + n)
            up = dot(a_ref[...], w_ref[:, at])
            by_gate, by_up, silu = gated_back(by_ref[:, at].astype(F32), gate_ref[:, at], up)
            act_ref[:, at], by_gate_ref[:, at], by_up_ref[:, at] = (silu * up).astype(BF), by_gate, by_up

    outs = [jax.ShapeDtypeStruct((tokens, f), BF)] * 3
    return kernel(f"up_back{number}", number, tokens // TILE, compute, [a, w, gate, by_act], [rows(d), whole(w.shape), rows(f), rows(f)], outs, [rows(f)] * 3, (), comm, schedule, 2 * tokens * d * f)


def gated_back_kernel(number, by_y, w, gate, up, comm=None, schedule=()):
    (tokens, d), f = by_y.shape, w.shape[0]

    def compute(step, i, o, _):
        by_ref, w_ref, gate_ref, up_ref = i
        for c, n in chunks(f):
            at = slice(c, c + n)
            by_act = dot_turned(by_ref[...], w_ref[at, :]).astype(BF).astype(F32)
            o[0][:, at], o[1][:, at], _ = gated_back(by_act, gate_ref[:, at], up_ref[:, at])

    outs = [jax.ShapeDtypeStruct((tokens, f), BF)] * 2
    return kernel(f"gated_back{number}", number, tokens // TILE, compute, [by_y, w, gate, up], [rows(d), whole(w.shape), rows(f), rows(f)], outs, [rows(f)] * 2, (), comm, schedule, 2 * tokens * d * f)


def state_back_kernel(number, by_gate, by_up, w_gate, w_up, h, by_y, comm=None, schedule=()):
    (tokens, f), d = by_gate.shape, h.shape[1]

    def compute(step, i, o, _):
        by_gate_ref, by_up_ref, w_gate_ref, w_up_ref, h_ref, by_ref = i
        by_a = dot_turned(by_gate_ref[...], w_gate_ref[...]).astype(BF).astype(F32)
        by_a = (by_a + dot_turned(by_up_ref[...], w_up_ref[...]).astype(BF).astype(F32)).astype(BF).astype(F32)
        wide = h_ref[...].astype(F32)
        scale = lax.rsqrt(jnp.mean(wide**2, -1, keepdims=True) + 1e-6)
        along = jnp.mean(by_a * wide, -1, keepdims=True) * scale * scale * scale
        by_h = (by_a * scale - wide * along).astype(BF)
        o[0][...] = (by_ref[...].astype(F32) + by_h.astype(F32)).astype(BF)

    outs = [jax.ShapeDtypeStruct((tokens, d), BF)]
    specs = [rows(f), rows(f), whole(w_gate.shape), whole(w_up.shape), rows(d), rows(d)]
    return kernel(f"state_back{number}", number, tokens // TILE, compute, [by_gate, by_up, w_gate, w_up, h, by_y], specs, outs, [rows(d)], (), comm, schedule, 4 * tokens * d * f)


def weight_back_kernel(number, x, y, comm=None, schedule=(), tile=640):
    (tokens, m), n = x.shape, y.shape[1]
    if n > m:
        inner = m // 256

        def compute(step, i, o, _):
            at = pl.ds(pl.multiple_of(step % inner * 256, 256), 256)
            o[0][...] = lax.dot_general(i[0][:, at], i[1][...], SUMMED, preferred_element_type=F32).astype(BF)

        grid = n // tile * inner
        specs = [whole(x.shape), pl.BlockSpec((tokens, tile), lambda s: (0, s // inner))]
        out_spec = pl.BlockSpec((256, tile), lambda s: (s % inner, s // inner))
    else:
        tile = 128

        def compute(step, i, o, _):
            o[0][...] = lax.dot_general(i[0][...], i[1][...], SUMMED, preferred_element_type=F32).astype(BF)

        grid = m // tile
        specs = [pl.BlockSpec((tokens, tile), lambda s: (0, s)), whole(y.shape)]
        out_spec = pl.BlockSpec((tile, n), lambda s: (s, 0))
    outs = [jax.ShapeDtypeStruct((m, n), BF)]
    return kernel(f"weight_back{number}", number, grid, compute, [x, y], specs, outs, [out_spec], (), comm, schedule, 2 * tokens * m * n)


class Butterfly:
    def __init__(self, x):
        self.inputs = [x]
        self.outputs = [jax.ShapeDtypeStruct(x.shape, F32)]
        self.out_specs = [pl.BlockSpec(x.shape, lambda *_: (0, 0))]
        self.scratch = [pltpu.VMEM((5,) + x.shape, F32), pltpu.VMEM((4,) + x.shape, F32), DMA((1,)), DMA((4,)), DMA((4,))]

    def phases(self, inputs, outputs, scratch):
        (x,), (out,), (held, arrived, local, send, recv) = inputs, outputs, scratch
        bits, me = position()

        def only():
            load = pltpu.make_async_copy(x, held.at[0], local.at[0])
            load.start()
            greet(bits, me)
            load.wait()
            for k, axis in enumerate((3, 0, 1, 2)):
                copy = pltpu.make_async_remote_copy(held.at[k], arrived.at[k], send.at[k], recv.at[k], device_id=across(bits, me, axis), device_id_type=pl.DeviceIdType.MESH)
                copy.start()
                copy.wait()
                held[k + 1] = held[k] + arrived[k]
            out[...] = held[4]

        return [only]


def adamw(w, m, v, g):
    m = 0.9 * m + 0.1 * g
    v = 0.95 * v + 0.05 * g * g
    step = m * lax.rsqrt(v + 1e-8) + 0.1 * w
    return (w - 0.02 * step).astype(BF), m, v


def clipped(gradients, sum_of_squares, count):
    factor = jnp.minimum(1.0, 0.5 * lax.rsqrt(sum_of_squares / count + 1e-30))
    return [g * factor for g in gradients]


FETCH = (0, 3, 7)
SUM = (0, 4, 7, 12, 17)
SUM8 = (0, 2, 3, 5, 7)


def solution(mesh):
    def cut(g):
        return g.reshape(2, 2, 2, 2, g.shape[0] // 16, g.shape[1])

    def joined(w):
        return w.reshape(-1, w.shape[-1])

    def step(x, dy, *arrays):
        weights, m, v = (arrays[i : i + 3] for i in (0, 3, 6))
        gates, ups, downs = weights
        h0, by_y = x[0], dy[0]
        (g0,) = kernel("fetch", 1, 1, None, [], [], [], [], comm=Gather(gates, 0))
        g0 = joined(g0)
        a0, gate0, u0 = gate_kernel(2, h0, g0, Gather(ups, 0), FETCH)
        up0, act0, d0 = up_kernel(3, a0, joined(u0), gate0, Gather(downs, 0), FETCH)
        h1, g1 = down_kernel(4, act0, joined(d0), h0, Gather(gates, 1), FETCH)
        g1 = joined(g1)
        a1, gate1, d1 = gate_kernel(5, h1, g1, Gather(downs, 1), FETCH)
        by_act1, u1 = hidden_back_kernel(6, by_y, joined(d1), Gather(ups, 1), FETCH)
        u1 = joined(u1)
        act1, by_gate1, by_up1 = up_back_kernel(7, a1, u1, gate1, by_act1)
        (by_d1,) = weight_back_kernel(8, act1, by_y)
        by_g1, sum_d1 = weight_back_kernel(9, a1, by_gate1, Scatter(cut(by_d1)), SUM)
        (by_u1,) = weight_back_kernel(10, a1, by_up1)
        by_h1, sum_g1 = state_back_kernel(11, by_gate1, by_up1, g1, u1, h1, by_y, Scatter(cut(by_g1)), SUM8)
        by_gate0, by_up0, sum_u1 = gated_back_kernel(12, by_h1, joined(d0), gate0, up0, Scatter(cut(by_u1)), SUM8)
        (by_d0,) = weight_back_kernel(13, act0, by_h1)
        by_g0, sum_d0 = weight_back_kernel(14, a0, by_gate0, Scatter(cut(by_d0)), SUM)
        by_u0, sum_g0 = weight_back_kernel(15, a0, by_up0, Scatter(cut(by_g0)), SUM)
        (sum_u0,) = kernel("add", 16, 1, None, [], [], [], [], comm=Scatter(cut(by_u0), 3))
        gradients = [jnp.stack(pair).astype(F32) for pair in ((sum_g0, sum_g1), (sum_u0, sum_u1), (sum_d0, sum_d1))]
        squares = sum(jnp.sum(g * g) for g in gradients)
        (squares,) = kernel("squares", 17, 1, None, [], [], [], [], comm=Butterfly(jnp.broadcast_to(squares, (8, 128))))
        gradients = clipped(gradients, squares[0, 0], 16 * sum(g.size for g in gradients))
        new = [adamw(w.astype(F32), m, v, g) for w, m, v, g in zip(weights, m, v, gradients, strict=True)]
        return tuple(one[which] for which in range(3) for one in new)

    states, block = P(("rep", "dp"), None, None), P(None, "dp", None)
    return jax.shard_map(
        step,
        mesh=mesh,
        in_specs=(states, states) + (block,) * 9,
        out_specs=(P("rep", "dp", None),) * 9,
        check_vma=False,
    )
```

```python
import functools

import jax
import jax.numpy as jnp
from jax import lax
from jax.experimental import pallas as pl
from jax.experimental.pallas import tpu as pltpu
from jax.sharding import PartitionSpec as P

BF, F32 = jnp.bfloat16, jnp.float32
ALL = pl.BlockSpec(memory_space=pl.ANY)
DMA = pltpu.SemaphoreType.DMA


def position():
    me = lax.axis_index("dp")
    return [(me // w) % 2 for w in (8, 4, 2, 1)], me


def across(bits, me, axis):
    w = (8, 4, 2, 1)[axis]
    return {"dp": me + w - 2 * w * bits[axis]}


def greet(bits, me):
    barrier = pltpu.get_barrier_semaphore()
    for axis in range(4):
        pl.semaphore_signal(barrier, inc=1, device_id=across(bits, me, axis), device_id_type=pl.DeviceIdType.MESH)
    pl.semaphore_wait(barrier, 4)


ORDERS = ((0, 1, 2), (1, 2, 0), (2, 0, 1))


def parts_of(columns, pieces):
    lanes, start, result = columns // 128, 0, []
    for j in range(pieces):
        piece = []
        for p, order in enumerate(ORDERS):
            mine = (lanes + 2 - p) // 3
            n = 128 * (mine * (j + 1) // pieces - mine * j // pieces)
            if n:
                piece.append((start, n, order))
            start += n
        result.append(piece)
    return result


class Gather:
    def __init__(self, source, layer, pieces=2):
        self.source, self.layer = source, layer
        self.rows, self.columns = source.shape[1:]
        self.pieces = parts_of(self.columns, pieces)
        self.inputs = [source]
        self.outputs = [jax.ShapeDtypeStruct((2, 2, 2, 2, self.rows, self.columns), BF)]
        self.out_specs = [ALL]
        n = pieces
        self.scratch = [pltpu.VMEM((self.rows, self.columns), BF), DMA((2,)), DMA((n, 3, 3)), DMA((n, 3, 3)), DMA((n, 3, 3)), DMA((n, 3, 3)), DMA((2,))]

    def phases(self, inputs, outputs, scratch):
        (source,), (out,), (own, local, send, recv, csend, crecv, cown) = inputs, outputs, scratch
        bits, me = position()
        count = len(self.pieces)

        def region(flipped, both):
            return tuple(slice(None) if a in both else (1 - bits[a] if a in flipped else bits[a]) for a in range(4))

        def remote(src, dst, send_sem, recv_sem, axis):
            return pltpu.make_async_remote_copy(src, dst, send_sem, recv_sem, device_id=across(bits, me, axis), device_id_type=pl.DeviceIdType.MESH)

        def hop(j, p, stage):
            c0, n, order = self.pieces[j][p]
            where = region((), order[:stage]) + (slice(None), pl.ds(c0, n))
            src = own.at[:, pl.ds(c0, n)] if stage == 0 else out.at[where]
            return remote(src, out.at[where], send.at[j, p, stage], recv.at[j, p, stage], order[stage])

        def pass_on(j, p, stage):
            c0, n, order = self.pieces[j][p]
            where = region((order[stage],), order[:stage]) + (slice(None), pl.ds(c0, n))
            return remote(out.at[where], out.at[where], csend.at[j, p, stage], crecv.at[j, p, stage], 3)

        load = pltpu.make_async_copy(source.at[self.layer], own, local.at[0])
        store = pltpu.make_async_copy(own, out.at[tuple(bits)], local.at[1])
        give = remote(own, out.at[tuple(bits)], cown.at[0], cown.at[1], 3)

        def first():
            load.start()
            greet(bits, me)
            load.wait()
            for j in range(count):
                for p in range(len(self.pieces[j])):
                    hop(j, p, 0).start()
            store.start()
            give.start()

        def middle(j, stage):
            if stage == 1 and j == 0:
                store.wait()
            for p in range(len(self.pieces[j])):
                hop(j, p, stage - 1).wait_recv()
                if stage < 3:
                    hop(j, p, stage).start()
            for p in range(len(self.pieces[j])):
                pass_on(j, p, stage - 1).start()

        def last():
            give.wait()
            for j in range(count):
                for p in range(len(self.pieces[j])):
                    for stage in range(3):
                        hop(j, p, stage).wait_send()
                        pass_on(j, p, stage).wait()

        return [first] + [functools.partial(middle, j, s) for s in (1, 2, 3) for j in range(count)] + [last]


class Scatter:
    def __init__(self, g, pieces=2):
        self.rows, self.columns = g.shape[4:]
        self.pieces = parts_of(self.columns, pieces)
        self.inputs = [g]
        r, c, n = self.rows, self.columns, pieces
        self.outputs = [jax.ShapeDtypeStruct((r, c), BF)]
        self.out_specs = [pl.BlockSpec((r, c), lambda *_: (0, 0))]
        buffers = [(2, 2, 2, r, c), (2, 2, 2, r, c), (2, 2, r, c), (2, r, c), (r, c), (2, 2, r, c), (2, r, c), (r, c)]
        self.scratch = [pltpu.VMEM(b, BF) for b in buffers] + [DMA((n,)), DMA((n, 2)), DMA((n, 3, 3)), DMA((n, 3, 3))]

    def phases(self, inputs, outputs, scratch):
        (g,), (out,) = inputs, outputs
        keep, far, in1, in2, in3, out1, out2, out3, local, core, send, recv = scratch
        ins, outs = (in1, in2, in3), (out1, out2, out3)
        bits, me = position()

        def columns_of(j):
            parts = self.pieces[j]
            return pl.ds(parts[0][0], sum(n for _, n, _ in parts))

        def load(j):
            at = columns_of(j)
            return pltpu.make_async_copy(g.at[:, :, :, bits[3], :, at], keep.at[:, :, :, :, at], local.at[j])

        def swap(j):
            at = columns_of(j)
            return pltpu.make_async_remote_copy(g.at[:, :, :, 1 - bits[3], :, at], far.at[:, :, :, :, at], core.at[j, 0], core.at[j, 1], device_id=across(bits, me, 3), device_id_type=pl.DeviceIdType.MESH)

        def hop(j, p, stage):
            c0, n, order = self.pieces[j][p]
            at = (slice(None),) * (2 - stage) + (slice(None), pl.ds(c0, n))
            return pltpu.make_async_remote_copy(outs[stage].at[at], ins[stage].at[at], send.at[j, p, stage], recv.at[j, p, stage], device_id=across(bits, me, order[stage]), device_id_type=pl.DeviceIdType.MESH)

        def total(part, stage, block):
            c0, n, order = part
            at = pl.ds(c0, n)
            xyz = [None] * 3
            for a, b in zip(order, block):
                xyz[a] = b
            where = tuple(xyz) + (slice(None), at)
            t = keep[where].astype(F32) + far[where].astype(F32)
            for s in range(stage):
                t = t + ins[s][tuple(block[s + 1 :]) + (slice(None), at)].astype(F32)
            return t

        def first():
            greet(bits, me)
            for j in range(len(self.pieces)):
                swap(j).start()
                load(j).start()

        def stage_of(j, stage):
            if stage == 0:
                load(j).wait()
                swap(j).wait_recv()
            for p, part in enumerate(self.pieces[j]):
                c0, n, order = part
                b = [bits[a] for a in order]
                if stage:
                    hop(j, p, stage - 1).wait_recv()
                if stage == 3:
                    out[:, pl.ds(c0, n)] = total(part, 3, b).astype(BF)
                    continue
                if stage == 2:
                    out3[:, pl.ds(c0, n)] = total(part, 2, b[:2] + [1 - b[2]]).astype(BF)
                else:
                    @pl.loop(0, 4 if stage == 0 else 2)
                    def _(i):
                        rest = [i // 2, i % 2] if stage == 0 else [i]
                        block = b[:stage] + [1 - b[stage]] + rest
                        outs[stage][tuple(rest) + (slice(None), pl.ds(c0, n))] = total(part, stage, block).astype(BF)
                hop(j, p, stage).start()

        def last():
            for j in range(len(self.pieces)):
                swap(j).wait_send()
                for p in range(len(self.pieces[j])):
                    for stage in range(3):
                        hop(j, p, stage).wait_send()

        middle = [functools.partial(stage_of, j, s) for s in range(4) for j in range(len(self.pieces))]
        return [first] + middle + [last]


def kernel(name, number, grid, ticks, compute, inputs, in_specs, outputs, out_specs, scratch=(), comm=None, times=(), length=1.0, flops=0):
    n_in, n_out = len(inputs), len(outputs)
    comms = [] if comm is None else list(comm) if isinstance(comm, (list, tuple)) else [comm]
    c_in, c_out = [x for c in comms for x in c.inputs], [x for c in comms for x in c.outputs]
    c_scratch = [x for c in comms for x in c.scratch]
    total_ticks = grid * ticks

    def body(*refs):
        step = pl.program_id(0)
        i, o = refs[:n_in], refs[n_in + len(c_in) : n_in + len(c_in) + n_out]
        ci, co = list(refs[n_in : n_in + len(c_in)]), list(refs[n_in + len(c_in) + n_out :][: len(c_out)])
        rest = list(refs[n_in + len(c_in) + n_out + len(c_out) :])
        own, cs = rest[: len(scratch)], rest[len(scratch) :]
        phases = []
        for c in comms:
            mine = [[l.pop(0) for _ in range(n)] for l, n in ((ci, len(c.inputs)), (co, len(c.outputs)), (cs, len(c.scratch)))]
            phases += c.phases(*mine)
        when = [-int(-t * total_ticks // length) for t in times][: len(phases)]
        when += [total_ticks] * (len(phases) - len(when))

        def tick(k):
            for phase, w in zip(phases, when):
                if w < total_ticks and w % ticks == k:
                    pl.when(step == w // ticks)(phase)

        if compute:
            compute(step, i, o, own, tick)

        @pl.when(step == grid - 1)
        def _():
            for phase, w in zip(phases, when):
                if w >= total_ticks:
                    phase()

    return pl.pallas_call(
        body,
        grid=(grid,),
        out_shape=list(outputs) + c_out,
        in_specs=list(in_specs) + [ALL] * len(c_in),
        out_specs=list(out_specs) + [s for c in comms for s in c.out_specs],
        scratch_shapes=list(scratch) + c_scratch,
        compiler_params=pltpu.CompilerParams(
            dimension_semantics=("arbitrary",),
            collective_id=number if comms else None,
            has_side_effects=bool(comms),
            vmem_limit_bytes=62 << 20,
        ),
        cost_estimate=pl.CostEstimate(flops=flops, bytes_accessed=0, transcendentals=0),
        name=name,
    )(*inputs, *c_in)
NAMES = ("w_gate", "w_up", "w_down")
TILE = 256
TICKS = 2
TURNED = (((1,), (1,)), ((), ()))
SUMMED = (((0,), (0,)), ((), ()))


def chunks(n, size=768):
    starts = list(range(0, n - size + 1, size))
    return [(s, (n if s == starts[-1] else s + size) - s) for s in starts]


def dot(a, b):
    return jnp.dot(a, b, preferred_element_type=F32)


def dot_turned(a, b):
    return lax.dot_general(a, b, TURNED, preferred_element_type=F32)


def rows(columns):
    return pl.BlockSpec((TILE, columns), lambda s: (s, 0))


def whole(shape):
    return pl.BlockSpec(shape, lambda s: (0, 0), pipeline_mode=pl.Buffered(1))


def gate_kernel(number, h, w, comm=None, times=(), length=20.0):
    (tokens, d), f = h.shape, w.shape[1]

    def compute(step, i, o, _, tick):
        h_ref, w_ref = i
        a_ref, gate_ref = o
        wide = h_ref[...].astype(F32)
        a = (wide * lax.rsqrt(jnp.mean(wide**2, -1, keepdims=True) + 1e-6)).astype(BF)
        a_ref[...] = a
        for k, (c, n) in enumerate(chunks(f)):
            tick(k)
            gate_ref[:, c : c + n] = dot(a, w_ref[:, c : c + n])

    outs = [jax.ShapeDtypeStruct((tokens, d), BF), jax.ShapeDtypeStruct((tokens, f), F32)]
    return kernel(f"gate{number}", number, tokens // TILE, TICKS, compute, [h, w], [rows(d), whole(w.shape)], outs, [rows(d), rows(f)], (), comm, times, length, 2 * tokens * d * f)


def up_kernel(number, a, w, gate, comm=None, times=(), length=20.0):
    (tokens, d), f = a.shape, w.shape[1]

    def compute(step, i, o, _, tick):
        a_ref, w_ref, gate_ref = i
        up_ref, act_ref = o
        for k, (c, n) in enumerate(chunks(f)):
            tick(k)
            at = slice(c, c + n)
            up = dot(a_ref[...], w_ref[:, at])
            up_ref[:, at] = up
            gate = gate_ref[:, at]
            act_ref[:, at] = (gate * sigmoid(gate) * up).astype(BF)

    outs = [jax.ShapeDtypeStruct((tokens, f), F32), jax.ShapeDtypeStruct((tokens, f), BF)]
    return kernel(f"up{number}", number, tokens // TILE, TICKS, compute, [a, w, gate], [rows(d), whole(w.shape), rows(f)], outs, [rows(f), rows(f)], (), comm, times, length, 2 * tokens * d * f)


def down_kernel(number, act, w, h, comm=None, times=(), length=20.0):
    (tokens, f), d = act.shape, w.shape[1]

    def compute(step, i, o, _, tick):
        act_ref, w_ref, h_ref = i
        for k in range(TICKS):
            tick(k)
            at = slice(k * d // TICKS, (k + 1) * d // TICKS)
            product = dot(act_ref[...], w_ref[:, at]).astype(BF)
            o[0][:, at] = (h_ref[:, at].astype(F32) + product.astype(F32)).astype(BF)

    outs = [jax.ShapeDtypeStruct((tokens, d), BF)]
    return kernel(f"down{number}", number, tokens // TILE, TICKS, compute, [act, w, h], [rows(f), whole(w.shape), rows(d)], outs, [rows(d)], (), comm, times, length, 2 * tokens * d * f)


def sigmoid(x):
    return 0.5 * jnp.tanh(0.5 * x) + 0.5


def gated_back(by_act, gate, up):
    s = sigmoid(gate)
    silu = gate * s
    return (by_act * up * (s + silu * (1.0 - s))).astype(BF), (by_act * silu).astype(BF), silu


def hidden_back_kernel(number, by_y, w, comm=None, times=(), length=20.0):
    (tokens, d), f = by_y.shape, w.shape[0]

    def compute(step, i, o, _, tick):
        for k, (c, n) in enumerate(chunks(f)):
            tick(k)
            o[0][:, c : c + n] = dot_turned(i[0][...], i[1][c : c + n, :]).astype(BF)

    outs = [jax.ShapeDtypeStruct((tokens, f), BF)]
    return kernel(f"hidden_back{number}", number, tokens // TILE, TICKS, compute, [by_y, w], [rows(d), whole(w.shape)], outs, [rows(f)], (), comm, times, length, 2 * tokens * d * f)


def up_back_kernel(number, a, w, gate, by_act, comm=None, times=(), length=20.0):
    (tokens, d), f = a.shape, w.shape[1]

    def compute(step, i, o, _, tick):
        a_ref, w_ref, gate_ref, by_ref = i
        act_ref, by_gate_ref, by_up_ref = o
        for k, (c, n) in enumerate(chunks(f)):
            tick(k)
            at = slice(c, c + n)
            up = dot(a_ref[...], w_ref[:, at])
            by_gate, by_up, silu = gated_back(by_ref[:, at].astype(F32), gate_ref[:, at], up)
            act_ref[:, at], by_gate_ref[:, at], by_up_ref[:, at] = (silu * up).astype(BF), by_gate, by_up

    outs = [jax.ShapeDtypeStruct((tokens, f), BF)] * 3
    return kernel(f"up_back{number}", number, tokens // TILE, TICKS, compute, [a, w, gate, by_act], [rows(d), whole(w.shape), rows(f), rows(f)], outs, [rows(f)] * 3, (), comm, times, length, 2 * tokens * d * f)


def gated_back_kernel(number, by_y, w, gate, up, comm=None, times=(), length=20.0):
    (tokens, d), f = by_y.shape, w.shape[0]

    def compute(step, i, o, _, tick):
        by_ref, w_ref, gate_ref, up_ref = i
        for k, (c, n) in enumerate(chunks(f)):
            tick(k)
            at = slice(c, c + n)
            by_act = dot_turned(by_ref[...], w_ref[at, :]).astype(BF).astype(F32)
            o[0][:, at], o[1][:, at], _ = gated_back(by_act, gate_ref[:, at], up_ref[:, at])

    outs = [jax.ShapeDtypeStruct((tokens, f), BF)] * 2
    return kernel(f"gated_back{number}", number, tokens // TILE, TICKS, compute, [by_y, w, gate, up], [rows(d), whole(w.shape), rows(f), rows(f)], outs, [rows(f)] * 2, (), comm, times, length, 2 * tokens * d * f)


def state_back_kernel(number, by_gate, by_up, w_gate, w_up, h, by_y, comm=None, times=(), length=20.0):
    (tokens, f), d = by_gate.shape, h.shape[1]

    def compute(step, i, o, scratch, tick):
        by_gate_ref, by_up_ref, w_gate_ref, w_up_ref, h_ref, by_ref = i
        for k in range(TICKS):
            tick(k)
            at = slice(k * d // TICKS, (k + 1) * d // TICKS)
            part = dot_turned(by_gate_ref[...], w_gate_ref[at, :]).astype(BF).astype(F32)
            part += dot_turned(by_up_ref[...], w_up_ref[at, :]).astype(BF).astype(F32)
            scratch[0][:, at] = part.astype(BF).astype(F32)
        by_a = scratch[0][...]
        wide = h_ref[...].astype(F32)
        scale = lax.rsqrt(jnp.mean(wide**2, -1, keepdims=True) + 1e-6)
        along = jnp.mean(by_a * wide, -1, keepdims=True) * scale * scale * scale
        by_h = (by_a * scale - wide * along).astype(BF)
        o[0][...] = (by_ref[...].astype(F32) + by_h.astype(F32)).astype(BF)

    outs = [jax.ShapeDtypeStruct((tokens, d), BF)]
    specs = [rows(f), rows(f), whole(w_gate.shape), whole(w_up.shape), rows(d), rows(d)]
    return kernel(f"state_back{number}", number, tokens // TILE, TICKS, compute, [by_gate, by_up, w_gate, w_up, h, by_y], specs, outs, [rows(d)], [pltpu.VMEM((TILE, d), F32)], comm, times, length, 4 * tokens * d * f)


def weight_back_kernel(number, x, y, comm=None, times=(), length=20.0, tile=640):
    (tokens, m), n = x.shape, y.shape[1]
    wide = n > m
    tiled, still = (y, x) if wide else (x, y)
    part = still.shape[1] // TICKS

    def compute(step, i, o, _, tick):
        for k in range(TICKS):
            tick(k)
            at = slice(k * part, (k + 1) * part)
            product = lax.dot_general(i[0][...], i[1][:, at], SUMMED, preferred_element_type=F32).astype(BF)
            if wide:
                o[0][at, :] = product.T
            else:
                o[0][:, at] = product

    specs = [pl.BlockSpec((tokens, tile), lambda s: (0, s)), whole(still.shape)]
    out_spec = pl.BlockSpec((m, tile), lambda s: (0, s)) if wide else pl.BlockSpec((tile, n), lambda s: (s, 0))
    outs = [jax.ShapeDtypeStruct((m, n), BF)]
    return kernel(f"weight_back{number}", number, tiled.shape[1] // tile, TICKS, compute, [tiled, still], specs, outs, [out_spec], (), comm, times, length, 2 * tokens * m * n)


class Butterfly:
    def __init__(self, x):
        self.inputs = [x]
        self.outputs = [jax.ShapeDtypeStruct(x.shape, F32)]
        self.out_specs = [pl.BlockSpec(x.shape, lambda *_: (0, 0))]
        self.scratch = [pltpu.VMEM((5,) + x.shape, F32), pltpu.VMEM((4,) + x.shape, F32), DMA((1,)), DMA((4,)), DMA((4,))]

    def phases(self, inputs, outputs, scratch):
        (x,), (out,), (held, arrived, local, send, recv) = inputs, outputs, scratch
        bits, me = position()

        def only():
            load = pltpu.make_async_copy(x, held.at[0], local.at[0])
            load.start()
            greet(bits, me)
            load.wait()
            for k, axis in enumerate((3, 0, 1, 2)):
                copy = pltpu.make_async_remote_copy(held.at[k], arrived.at[k], send.at[k], recv.at[k], device_id=across(bits, me, axis), device_id_type=pl.DeviceIdType.MESH)
                copy.start()
                copy.wait()
                held[k + 1] = held[k] + arrived[k]
            out[...] = held[4]

        return [only]


def adamw(w, m, v, g):
    m = 0.9 * m + 0.1 * g
    v = 0.95 * v + 0.05 * g * g
    step = m * lax.rsqrt(v + 1e-8) + 0.1 * w
    return (w - 0.02 * step).astype(BF), m, v


def clipped(gradients, sum_of_squares, count):
    factor = jnp.minimum(1.0, 0.5 * lax.rsqrt(sum_of_squares / count + 1e-30))
    return [g * factor for g in gradients]


FETCH = (0.0, 4.0, 5.5, 9.0, 12.0, 18.0)
SUM = (0.0, 5.5, 8.0, 14.0, 20.0, 22.0, 25.0, 28.0, 31.0)


def solution(mesh):
    def cut(g):
        return g.reshape(2, 2, 2, 2, g.shape[0] // 16, g.shape[1])

    def joined(w):
        return w.reshape(-1, w.shape[-1])

    def step(x, dy, *arrays):
        weights, m, v = (arrays[i : i + 3] for i in (0, 3, 6))
        gates, ups, downs = weights
        h0, by_y = x[0], dy[0]
        (g0,) = kernel("fetch", 1, 1, 1, None, [], [], [], [], comm=Gather(gates, 0, 3))
        g0 = joined(g0)
        a0, gate0, u0 = gate_kernel(2, h0, g0, Gather(ups, 0), FETCH, 21.0)
        up0, act0, d0 = up_kernel(3, a0, joined(u0), gate0, Gather(downs, 0), FETCH, 31.0)
        h1, g1 = down_kernel(4, act0, joined(d0), h0, Gather(gates, 1), FETCH, 21.0)
        g1 = joined(g1)
        a1, gate1, d1 = gate_kernel(5, h1, g1, Gather(downs, 1), FETCH, 21.0)
        by_act1, u1 = hidden_back_kernel(6, by_y, joined(d1), Gather(ups, 1), FETCH, 20.0)
        u1 = joined(u1)
        act1, by_gate1, by_up1 = up_back_kernel(7, a1, u1, gate1, by_act1)
        (by_d1,) = weight_back_kernel(8, act1, by_y)
        by_g1, sum_d1 = weight_back_kernel(9, a1, by_gate1, Scatter(cut(by_d1)), SUM, 20.0)
        (by_u1,) = weight_back_kernel(10, a1, by_up1)
        by_h1, sum_g1 = state_back_kernel(11, by_gate1, by_up1, g1, u1, h1, by_y, Scatter(cut(by_g1)), SUM, 40.0)
        by_gate0, by_up0, sum_u1 = gated_back_kernel(12, by_h1, joined(d0), gate0, up0, Scatter(cut(by_u1)), SUM, 38.0)
        (by_d0,) = weight_back_kernel(13, act0, by_h1)
        by_g0, sum_d0 = weight_back_kernel(14, a0, by_gate0, Scatter(cut(by_d0)), SUM, 20.0)
        by_u0, sum_g0 = weight_back_kernel(15, a0, by_up0, Scatter(cut(by_g0)), SUM, 20.0)
        (sum_u0,) = kernel("add", 16, 1, 1, None, [], [], [], [], comm=Scatter(cut(by_u0), 3))
        gradients = [jnp.stack(pair).astype(F32) for pair in ((sum_g0, sum_g1), (sum_u0, sum_u1), (sum_d0, sum_d1))]
        squares = sum(jnp.sum(g * g) for g in gradients)
        (squares,) = kernel("squares", 17, 1, 1, None, [], [], [], [], comm=Butterfly(jnp.broadcast_to(squares, (8, 128))))
        gradients = clipped(gradients, squares[0, 0], 16 * sum(g.size for g in gradients))
        new = [adamw(w.astype(F32), m, v, g) for w, m, v, g in zip(weights, m, v, gradients, strict=True)]
        return tuple(one[which] for which in range(3) for one in new)

    states, block = P(("rep", "dp"), None, None), P(None, "dp", None)
    return jax.shard_map(
        step,
        mesh=mesh,
        in_specs=(states, states) + (block,) * 9,
        out_specs=(P("rep", "dp", None),) * 9,
        check_vma=False,
    )
```
